32 devices in a mesh: ta: 1, gx: 8 (over y, x, core), gy: 4 (over z).
Axes of the slice: x: 2, y: 2, z: 4, core: 2. Of those that a mesh axis runs over, the one named last changes fastest.
Arguments:
- propagator: bfloat16 [1, 2, 4, 3, 4, 3, 64, 4096], P('ta', None, None, None, None, None, 'gx', 'gy'), may hold values from -1.5 to 1.5
- gamma_table: int32 [16, 8], replicated, may hold values from 0 to 3, as said below
Outputs:
- spectrum: float32 [1, 16, 64, 64, 128], P('ta', None, ('gx', 'gy'))
The draws below stay inside these ranges and needn't reach their ends.
Inputs may be any that keep to these rules, and one draw needn't show every extreme that they name: gamma_table[g, 0:4] is a permutation of 0 to 3, gamma_table[g, 4:8] are powers of i.
All inputs are finite; a program needn't handle non-finite values.
Results may differ from the reference program's by a relative error of at most 0.0061.
Values may be sent and summed in bfloat16 or wider, within the bound.
No kernel may reach another device: no remote copies, remote signals or barrier semaphores. Data moves between devices by JAX's collectives and lax.ppermute only.
A program may use at most 192 MiB of HBM per device.

```python
import math
import jax
import jax.numpy as jnp
from jax import lax

EXTENT = 64
CHANNELS = 16
SLICES = 1


def draw_gamma_table(key, part):
    subkeys = jax.random.split(key, CHANNELS)
    orders = jax.vmap(lambda subkey: jax.random.permutation(subkey, 4))(subkeys)
    phase_codes = jax.random.randint(jax.random.fold_in(key, 11), (CHANNELS, 4), 0, 4, dtype=jnp.int32)
    return jnp.concatenate([orders.astype(jnp.int32), phase_codes], axis=1)


def level_of(stream_key, extent, cuts, low, high):
    factor_of, own = 1.0, jax.random.fold_in(stream_key, 6)
    for position, blocks in cuts:
        steps = jnp.exp(jax.random.uniform(jax.random.fold_in(own, position), (blocks,), jnp.float32, low / len(cuts), high / len(cuts)))
        factor_of = factor_of * jnp.repeat(steps, extent[position] // blocks).reshape([-1 if axis == position else 1 for axis in range(len(extent))])
    return factor_of


def bell_draw(key, shape, deviation, reach, pieces=(), kind=jnp.bfloat16):
    factor_of = level_of(key, shape, pieces, -0.22, 0.18) if pieces else 1.0
    array = jax.random.normal(key, shape, jnp.float32) * deviation * factor_of
    return jnp.minimum(jnp.maximum(array, -reach), reach).astype(kind)


def setup_inputs(seed: int = 0) -> dict:
    key_of = jax.random.split(jax.random.key(seed), 3)
    propagator = bell_draw(key_of[0], (SLICES, 2, 4, 3, 4, 3, EXTENT, EXTENT * EXTENT), 0.25, 1.5, ((6, 8), (7, 4)))
    gamma_table = draw_gamma_table(jax.random.fold_in(key_of[2], 71), 0)
    return dict(propagator=propagator, gamma_table=gamma_table)


def precise_dot(left_matrix, right_matrix):
    return jnp.dot(left_matrix, right_matrix, precision=lax.Precision.HIGHEST, preferred_element_type=jnp.float32)

def channel_weights(channel_table):
    spin_index = jnp.arange(4, dtype=jnp.int32)
    targets = channel_table[:, :4]
    codes_all = channel_table[:, 4:]
    mapping = (targets[:, :, None] == spin_index[None, None, :]).astype(jnp.float32)
    phase_real = (codes_all == 0).astype(jnp.float32) - (codes_all == 2).astype(jnp.float32)
    phase_imag = (codes_all == 1).astype(jnp.float32) - (codes_all == 3).astype(jnp.float32)
    pair_real = phase_real[:, None, :] * phase_real[:, :, None] - phase_imag[:, None, :] * phase_imag[:, :, None]
    pair_imag = phase_real[:, None, :] * phase_imag[:, :, None] + phase_imag[:, None, :] * phase_real[:, :, None]
    source_map = jnp.transpose(mapping, (0, 2, 1))
    selector = source_map[:, :, None, :, None] * mapping[:, None, :, None, :]
    count_channels = channel_table.shape[0]
    weight_real = (pair_real[:, None, :, :, None] * selector).reshape(count_channels, 256)
    weight_imag = (pair_imag[:, None, :, :, None] * selector).reshape(count_channels, 256)
    return (weight_real, weight_imag)

def spin_products(field_real, field_imag):
    site_count = field_real.shape[-1]
    total_real = jnp.zeros((4, 4, 4, 4, site_count), jnp.float32)
    total_imag = jnp.zeros((4, 4, 4, 4, site_count), jnp.float32)
    for color_in in range(3):
        for color_out in range(3):
            left_real = field_real[:, color_in, :, color_out].astype(jnp.float32)
            left_imag = field_imag[:, color_in, :, color_out].astype(jnp.float32)
            total_real = total_real + left_real[:, :, None, None] * left_real[None, None] + left_imag[:, :, None, None] * left_imag[None, None]
            total_imag = total_imag + left_imag[:, :, None, None] * left_real[None, None] - left_real[:, :, None, None] * left_imag[None, None]
    return (total_real.reshape(256, site_count), total_imag.reshape(256, site_count))

def dft_tables(length):
    steps_index = jnp.arange(length, dtype=jnp.int32)
    phases = steps_index[:, None] * steps_index[None, :] % length
    angles = phases.astype(jnp.float32) * (2.0 * math.pi / length)
    norm_factor = 1.0 / math.sqrt(length)
    cosine = (jnp.cos(angles) * norm_factor).astype(jnp.bfloat16)
    sine_table = (jnp.sin(angles) * norm_factor).astype(jnp.bfloat16)
    return (cosine.astype(jnp.float32), sine_table.astype(jnp.float32))

def section(complex_pair, which_axis, cosine, sine_table):
    field_real = complex_pair[0].astype(jnp.float32)
    field_imag = complex_pair[1].astype(jnp.float32)

    def contract_axis(values, weights):
        moved = jnp.tensordot(values, weights, axes=([which_axis], [0]), precision=lax.Precision.HIGHEST)
        return jnp.moveaxis(moved, -1, which_axis)
    new_real = contract_axis(field_real, cosine) + contract_axis(field_imag, sine_table)
    new_imag = contract_axis(field_imag, cosine) - contract_axis(field_real, sine_table)
    return (new_real, new_imag)

def to_half(complex_pair):
    return lax.optimization_barrier((complex_pair[0].astype(jnp.bfloat16), complex_pair[1].astype(jnp.bfloat16)))

def reference(propagator, gamma_table):
    weight_real, weight_imag = channel_weights(gamma_table)
    stack_real = jnp.concatenate([weight_real, -weight_imag], axis=1)
    stack_imag = jnp.concatenate([weight_imag, weight_real], axis=1)
    cosine, sine_table = dft_tables(EXTENT)
    volume = EXTENT ** 3

    def one_slice(slice_block):
        flattened = slice_block.astype(jnp.float32).reshape(2, 4, 3, 4, 3, volume)
        prod_real, prod_imag = spin_products(flattened[0], flattened[1])
        prod_stack = jnp.concatenate([prod_real, prod_imag], axis=0).astype(jnp.bfloat16)
        prod_stack = lax.optimization_barrier(prod_stack).astype(jnp.float32)
        dens_real = precise_dot(stack_real, prod_stack).reshape(-1, EXTENT, EXTENT, EXTENT)
        dens_imag = precise_dot(stack_imag, prod_stack).reshape(-1, EXTENT, EXTENT, EXTENT)
        pair = to_half((dens_real, dens_imag))
        pair = to_half(section(pair, 3, cosine, sine_table))
        pair = to_half(section(pair, 2, cosine, sine_table))
        spec_real, spec_imag = section(pair, 1, cosine, sine_table)
        spec_real = jnp.transpose(spec_real, (0, 3, 1, 2))
        spec_imag = jnp.transpose(spec_imag, (0, 3, 1, 2))
        return jnp.concatenate([spec_real, spec_imag], axis=3).astype(jnp.float32)
    return lax.map(one_slice, propagator)
```

```python
import functools
import math

import jax
import jax.numpy as jnp
import numpy as np
from jax import lax
from jax.experimental import pallas as pl
from jax.experimental.pallas import tpu as pltpu
from jax.sharding import PartitionSpec as P

LANES = 128
SPINS = 4
PAIRS = SPINS * SPINS
SLOTS = PAIRS * PAIRS


def dft_tables(length):
    index = np.arange(length)
    angles = (index[:, None] * index[None, :] % length) * (2.0 * math.pi / length)
    norm = 1.0 / math.sqrt(length)
    return np.cos(angles) * norm, np.sin(angles) * norm


def z_matrix(length, lane_rows, per_device):
    cosine, sine = dft_tables(length)
    mix = np.array([[cosine, sine], [-sine, cosine]])
    eye = np.eye(lane_rows)
    full = np.einsum("oizk,yv->koyivz", mix, eye)
    return full.reshape(length * 2 * lane_rows, 2 * lane_rows * length)


def y_matrix(length, grid_y, steps, lane_rows, per_device):
    cosine, sine = dft_tables(length)
    cosine = cosine.reshape(grid_y, steps, lane_rows, length)
    sine = sine.reshape(grid_y, steps, lane_rows, length)
    real = np.stack([cosine, sine])
    imag = np.stack([-sine, cosine])
    plain = np.stack([real, imag])
    turned = np.stack([imag, -real])
    both = np.stack([plain, turned])
    full = np.einsum("aoigjvk,pq->gjpivaqok", both, np.eye(per_device))
    rows = grid_y * steps * per_device * 2 * lane_rows
    return full.reshape(rows, 2 * per_device * 2 * length)


def density_weights(table):
    count = table.shape[0]
    slot = lax.broadcasted_iota(jnp.int32, (count, SLOTS), 1)
    s1, s2, s3, s4 = (slot >> 6) & 3, (slot >> 4) & 3, (slot >> 2) & 3, slot & 3

    def pick(spin, base):
        value = jnp.broadcast_to(table[:, base : base + 1], (count, SLOTS))
        for q in range(1, SPINS):
            other = jnp.broadcast_to(table[:, base + q : base + q + 1], (count, SLOTS))
            value = jnp.where(spin == q, other, value)
        return value

    def weight(a1, a2, b1, b2):
        hit = (a1 == pick(b1, 0)) & (b2 == pick(a2, 0))
        code = (pick(b1, SPINS) + pick(a2, SPINS)) & 3
        real = jnp.where(code == 0, 1.0, 0.0) - jnp.where(code == 2, 1.0, 0.0)
        imag = jnp.where(code == 1, 1.0, 0.0) - jnp.where(code == 3, 1.0, 0.0)
        return jnp.where(hit, real, 0.0), jnp.where(hit, imag, 0.0)

    here_r, here_i = weight(s1, s2, s3, s4)
    swap_r, swap_i = weight(s3, s4, s1, s2)
    first, second = slot >> 4, slot & 15
    upper, diagonal = first < second, first == second
    real = jnp.where(diagonal, here_r, jnp.where(upper, here_r + swap_r, here_i - swap_i))
    imag = jnp.where(diagonal, here_i, jnp.where(upper, here_i + swap_i, swap_r - here_r))
    return jnp.concatenate([real, imag], axis=0)


def front_kernel(prop, table, zmat, out, weights, gram, *, tiles, colors, rows_x, owners):
    @pl.when((pl.program_id(0) == 0) & (pl.program_id(1) == 0))
    def _():
        weights[...] = density_weights(table[...]).astype(jnp.bfloat16)

    channels = weights.shape[0] // 2
    pieces = []
    for tile in range(tiles):
        lanes = pl.ds(tile * LANES, LANES)

        def site(part, pair, tile_lanes=lanes):
            s1, s2 = divmod(pair, SPINS)
            return [
                prop[0, part, s1, c1, s2, c2, :, tile_lanes].astype(jnp.float32)
                for c1 in range(colors)
                for c2 in range(colors)
            ]

        def put(a, b, value, tile=tile):
            gram[tile, pl.ds((a * PAIRS + b) * rows_x, rows_x), :] = value

        def total(left, right):
            acc = left[0] * right[0]
            for x, y in zip(left[1:], right[1:]):
                acc = acc + x * y
            return acc

        for a in range(PAIRS):
            ar, ai = site(0, a), site(1, a)
            asum = [x + y for x, y in zip(ar, ai)]
            put(a, a, total(ar, ar) + total(ai, ai))
            for b in range(a + 1, PAIRS):
                br, bi = site(0, b), site(1, b)
                p, q = total(ar, br), total(ai, bi)
                t = total(asum, [x - y for x, y in zip(br, bi)])
                put(a, b, p + q)
                put(b, a, (t - p) + q)
        for x in range(rows_x):
            products = gram[tile, pl.ds(x, SLOTS, stride=rows_x), :].astype(jnp.bfloat16)
            dens = jnp.dot(weights[...], products, preferred_element_type=jnp.float32)
            dens = dens.astype(jnp.bfloat16)
            pieces.append(jnp.concatenate([dens[:channels], dens[channels:]], axis=1))
    stacked = jnp.concatenate(pieces, axis=0)
    turned = lax.dot_general(
        zmat[...], stacked, (((1,), (1,)), ((), ())), preferred_element_type=jnp.float32
    )
    width = rows_x * channels
    rows = turned.shape[0] // owners
    turned = turned.reshape(owners, rows, tiles * width)
    out[0] = jnp.concatenate(
        [turned[:, :, k * width : (k + 1) * width] for k in range(tiles)], axis=1
    ).astype(jnp.bfloat16)


def back_kernel(data, ymat, xmat, out, lined, *, grid_x, rows_x, channels, pitch, per_device):
    cols = ymat.shape[1]
    blocks = cols // LANES
    for gx in range(grid_x):
        turned = lax.dot_general(
            data[0, gx], ymat[...], (((0,), (0,)), ((), ())), preferred_element_type=jnp.float32
        )
        for block in range(blocks):
            for x in range(rows_x):
                lined[block, gx, pl.ds(x * pitch, channels), :] = turned[
                    x * channels : (x + 1) * channels, block * LANES : (block + 1) * LANES
                ]
    for c in range(channels):
        sides = []
        for block in range(blocks):
            lines = [
                lined[block, gx, pl.ds(c, rows_x, stride=pitch), :] for gx in range(grid_x)
            ]
            sides.append(jnp.concatenate(lines, axis=0).astype(jnp.bfloat16))
        half = blocks // 2
        right = jnp.concatenate(
            [jnp.concatenate(sides[:half], axis=1), jnp.concatenate(sides[half:], axis=1)], axis=0
        )
        spectrum = jnp.dot(xmat[...], right, preferred_element_type=jnp.float32)
        width = cols // 2 // per_device
        for k in range(per_device):
            out[0, c, k] = spectrum[:, k * width : (k + 1) * width]


def body(propagator, gamma_table):
    slices, _, _, colors, _, _, rows_x, cols_yz = propagator.shape
    channels = gamma_table.shape[0]
    grid_x, grid_y = lax.axis_size("gx"), lax.axis_size("gy")
    owners = grid_x * grid_y
    extent = rows_x * grid_x
    per_device = extent // owners
    lane_rows = LANES // extent
    steps = cols_yz // LANES
    tiles = 2
    zmat = jnp.asarray(z_matrix(extent, lane_rows, per_device), jnp.bfloat16)
    ymat = jnp.asarray(y_matrix(extent, grid_y, steps, lane_rows, per_device), jnp.bfloat16)
    cosine, sine = dft_tables(extent)
    xmat = jnp.asarray(np.concatenate([cosine.T, sine.T], axis=1), jnp.bfloat16)

    width = rows_x * channels
    rows = steps * per_device * 2 * lane_rows
    step_rows = tiles * per_device * 2 * lane_rows
    sent = pl.pallas_call(
        functools.partial(
            front_kernel, tiles=tiles, colors=colors, rows_x=rows_x, owners=owners
        ),
        grid=(slices, steps // tiles),
        in_specs=[
            pl.BlockSpec(
                (1, 2, SPINS, colors, SPINS, colors, rows_x, tiles * LANES),
                lambda t, j: (t, 0, 0, 0, 0, 0, 0, j),
            ),
            pl.BlockSpec(gamma_table.shape, lambda t, j: (0, 0)),
            pl.BlockSpec(zmat.shape, lambda t, j: (0, 0)),
        ],
        out_specs=pl.BlockSpec((1, owners, step_rows, width), lambda t, j: (t, 0, j, 0)),
        out_shape=jax.ShapeDtypeStruct((slices, owners, rows, width), jnp.bfloat16),
        scratch_shapes=[
            pltpu.VMEM((2 * channels, SLOTS), jnp.bfloat16),
            pltpu.VMEM((tiles, SLOTS * rows_x, LANES), jnp.float32),
        ],
        name="front",
    )(propagator, gamma_table, zmat)

    got = lax.all_to_all(sent, ("gx", "gy"), split_axis=1, concat_axis=1, tiled=True)
    got = got.reshape(slices, grid_x, grid_y * rows, width)

    pitch = channels + 8
    return pl.pallas_call(
        functools.partial(
            back_kernel,
            grid_x=grid_x,
            rows_x=rows_x,
            channels=channels,
            pitch=pitch,
            per_device=per_device,
        ),
        grid=(slices,),
        in_specs=[
            pl.BlockSpec((1, grid_x, grid_y * rows, width), lambda t: (t, 0, 0, 0)),
            pl.BlockSpec(ymat.shape, lambda t: (0, 0)),
            pl.BlockSpec(xmat.shape, lambda t: (0, 0)),
        ],
        out_specs=pl.BlockSpec(
            (1, channels, per_device, extent, 2 * extent), lambda t: (t, 0, 0, 0, 0)
        ),
        out_shape=jax.ShapeDtypeStruct(
            (slices, channels, per_device, extent, 2 * extent), jnp.float32
        ),
        scratch_shapes=[
            pltpu.VMEM((ymat.shape[1] // LANES, grid_x, rows_x * pitch, LANES), jnp.float32)
        ],
        name="back",
    )(got, ymat, xmat)


def solution(mesh):
    return jax.shard_map(
        body,
        mesh=mesh,
        in_specs=(P("ta", None, None, None, None, None, "gx", "gy"), P()),
        out_specs=P("ta", None, ("gx", "gy"), None, None),
        check_vma=False,
    )
```

```python
import functools
import math

import jax
import jax.numpy as jnp
import numpy as np
from jax import lax
from jax.experimental import pallas as pl
from jax.experimental.pallas import tpu as pltpu
from jax.sharding import PartitionSpec as P

LANES = 128
SPINS = 4
PAIRS = SPINS * SPINS
SLOTS = PAIRS * PAIRS


def dft_tables(length):
    index = np.arange(length)
    angles = (index[:, None] * index[None, :] % length) * (2.0 * math.pi / length)
    norm = 1.0 / math.sqrt(length)
    return np.cos(angles) * norm, np.sin(angles) * norm


def z_matrix(length, lane_rows, per_device):
    cosine, sine = dft_tables(length)
    mix = np.array([[cosine, sine], [-sine, cosine]])
    eye = np.eye(lane_rows)
    full = np.einsum("oizk,yv->koyivz", mix, eye)
    return full.reshape(length * 2 * lane_rows, 2 * lane_rows * length)


def y_matrix(length, grid_y, steps, lane_rows, per_device):
    cosine, sine = dft_tables(length)
    cosine = cosine.reshape(grid_y, steps, lane_rows, length)
    sine = sine.reshape(grid_y, steps, lane_rows, length)
    real = np.stack([cosine, sine])
    imag = np.stack([-sine, cosine])
    plain = np.stack([real, imag])
    turned = np.stack([imag, -real])
    both = np.stack([plain, turned])
    full = np.einsum("aoigjvk,pq->gjpivaqok", both, np.eye(per_device))
    rows = grid_y * steps * per_device * 2 * lane_rows
    return full.reshape(rows, 2 * per_device * 2 * length)


def density_weights(table):
    count = table.shape[0]
    slot = lax.broadcasted_iota(jnp.int32, (count, SLOTS), 1)
    first, step = slot >> 4, slot & 15
    is_real = (step < 8) | ((step == 8) & (first < 8))
    second = (first + jnp.where(step > 8, step - 8, step)) & 15
    s1, s2, s3, s4 = first >> 2, first & 3, second >> 2, second & 3

    def pick(spin, base):
        value = jnp.broadcast_to(table[:, base : base + 1], (count, SLOTS))
        for q in range(1, SPINS):
            other = jnp.broadcast_to(table[:, base + q : base + q + 1], (count, SLOTS))
            value = jnp.where(spin == q, other, value)
        return value

    def weight(a1, a2, b1, b2):
        hit = (a1 == pick(b1, 0)) & (b2 == pick(a2, 0))
        code = (pick(b1, SPINS) + pick(a2, SPINS)) & 3
        real = jnp.where(code == 0, 1.0, 0.0) - jnp.where(code == 2, 1.0, 0.0)
        imag = jnp.where(code == 1, 1.0, 0.0) - jnp.where(code == 3, 1.0, 0.0)
        return jnp.where(hit, real, 0.0), jnp.where(hit, imag, 0.0)

    here_r, here_i = weight(s1, s2, s3, s4)
    swap_r, swap_i = weight(s3, s4, s1, s2)
    single = step == 0
    real = jnp.where(single, here_r, jnp.where(is_real, here_r + swap_r, swap_i - here_i))
    imag = jnp.where(single, here_i, jnp.where(is_real, here_i + swap_i, here_r - swap_r))
    return jnp.concatenate([real, imag], axis=0)


def front_kernel(prop, table, zmat, out, weights, packed, gram, *, tiles, colors, rows_x, owners):
    @pl.when((pl.program_id(0) == 0) & (pl.program_id(1) == 0))
    def _():
        weights[...] = density_weights(jnp.transpose(table[...])).astype(jnp.bfloat16)

    channels = weights.shape[0] // 2
    spread = colors * colors
    for pair in range(PAIRS):
        s1, s2 = divmod(pair, SPINS)
        for color in range(spread):
            c1, c2 = divmod(color, colors)
            for part in range(2):
                wide = prop[0, part, s1, c1, s2, c2, :, :].astype(jnp.float32)
                both = jnp.concatenate(
                    [wide[:, k * LANES : (k + 1) * LANES] for k in range(tiles)], axis=0
                )
                packed[part, pair, color] = both.astype(jnp.bfloat16)
                if part == 0:
                    packed[2, pair, color] = (-both).astype(jnp.bfloat16)

    def row(a, carry):
        def load(part, pair):
            return [packed[part, pair, color].astype(jnp.float32) for color in range(spread)]

        def total(left, right):
            acc = left[0] * right[0]
            for x, y in zip(left[1:], right[1:]):
                acc = acc + x * y
            return acc

        def put(d, value):
            start = pl.multiple_of((a * PAIRS + d) * rows_x, rows_x)
            for tile in range(tiles):
                gram[tile, pl.ds(start, rows_x), :] = value[tile * rows_x : (tile + 1) * rows_x]

        ar, ai, an = load(0, a), load(1, a), load(2, a)
        put(0, total(ar + ai, ar + ai))
        for d in range(1, PAIRS // 2 + 1):
            b = (a + d) & (PAIRS - 1)
            br, bi = load(0, b), load(1, b)
            real, imag = total(ar + ai, br + bi), total(ai + an, br + bi)
            if d < PAIRS // 2:
                put(d, real)
                put(d + PAIRS // 2, imag)
            else:
                put(d, jnp.where(a < PAIRS // 2, real, imag))
        return carry

    lax.fori_loop(0, PAIRS, row, 0)

    pieces = []
    for tile in range(tiles):
        for x in range(rows_x):
            products = gram[tile, pl.ds(x, SLOTS, stride=rows_x), :].astype(jnp.bfloat16)
            dens = jnp.dot(weights[...], products, preferred_element_type=jnp.float32)
            dens = dens.astype(jnp.bfloat16)
            pieces.append(jnp.concatenate([dens[:channels], dens[channels:]], axis=1))
    stacked = jnp.concatenate(pieces, axis=0)
    turned = lax.dot_general(
        zmat[...], stacked, (((1,), (1,)), ((), ())), preferred_element_type=jnp.float32
    )
    width = rows_x * channels
    rows = turned.shape[0] // owners
    turned = turned.reshape(owners, rows, tiles * width)
    out[0] = jnp.concatenate(
        [turned[:, :, k * width : (k + 1) * width] for k in range(tiles)], axis=1
    ).astype(jnp.bfloat16)


def back_kernel(data, ymat, xmat, out, lined, *, grid_x, rows_x, channels, pitch, per_device):
    cols = ymat.shape[1]
    blocks = cols // LANES
    for gx in range(grid_x):
        turned = lax.dot_general(
            data[0, gx], ymat[...], (((0,), (0,)), ((), ())), preferred_element_type=jnp.float32
        )
        for block in range(blocks):
            for x in range(rows_x):
                lined[block, gx, pl.ds(x * pitch, channels), :] = turned[
                    x * channels : (x + 1) * channels, block * LANES : (block + 1) * LANES
                ]
    for c in range(channels):
        sides = []
        for block in range(blocks):
            lines = [
                lined[block, gx, pl.ds(c, rows_x, stride=pitch), :] for gx in range(grid_x)
            ]
            sides.append(jnp.concatenate(lines, axis=0).astype(jnp.bfloat16))
        half = blocks // 2
        right = jnp.concatenate(
            [jnp.concatenate(sides[:half], axis=1), jnp.concatenate(sides[half:], axis=1)], axis=0
        )
        spectrum = jnp.dot(xmat[...], right, preferred_element_type=jnp.float32)
        width = cols // 2 // per_device
        for k in range(per_device):
            out[0, c, k] = spectrum[:, k * width : (k + 1) * width]


def body(propagator, gamma_table):
    slices, _, _, colors, _, _, rows_x, cols_yz = propagator.shape
    channels = gamma_table.shape[0]
    grid_x, grid_y = lax.axis_size("gx"), lax.axis_size("gy")
    owners = grid_x * grid_y
    extent = rows_x * grid_x
    per_device = extent // owners
    lane_rows = LANES // extent
    steps = cols_yz // LANES
    tiles = 2
    zmat = jnp.asarray(z_matrix(extent, lane_rows, per_device), jnp.bfloat16)
    ymat = jnp.asarray(y_matrix(extent, grid_y, steps, lane_rows, per_device), jnp.bfloat16)
    cosine, sine = dft_tables(extent)
    xmat = jnp.asarray(np.concatenate([cosine.T, sine.T], axis=1), jnp.bfloat16)

    width = rows_x * channels
    rows = steps * per_device * 2 * lane_rows
    step_rows = tiles * per_device * 2 * lane_rows
    sent = pl.pallas_call(
        functools.partial(
            front_kernel, tiles=tiles, colors=colors, rows_x=rows_x, owners=owners
        ),
        grid=(slices, steps // tiles),
        in_specs=[
            pl.BlockSpec(
                (1, 2, SPINS, colors, SPINS, colors, rows_x, tiles * LANES),
                lambda t, j: (t, 0, 0, 0, 0, 0, 0, j),
            ),
            pl.BlockSpec(gamma_table.shape[::-1], lambda t, j: (0, 0)),
            pl.BlockSpec(zmat.shape, lambda t, j: (0, 0)),
        ],
        out_specs=pl.BlockSpec((1, owners, step_rows, width), lambda t, j: (t, 0, j, 0)),
        out_shape=jax.ShapeDtypeStruct((slices, owners, rows, width), jnp.bfloat16),
        scratch_shapes=[
            pltpu.VMEM((2 * channels, SLOTS), jnp.bfloat16),
            pltpu.VMEM((3, PAIRS, colors * colors, tiles * rows_x, LANES), jnp.bfloat16),
            pltpu.VMEM((tiles, SLOTS * rows_x, LANES), jnp.float32),
        ],
        name="front",
    )(propagator, gamma_table.T, zmat)

    got = lax.all_to_all(sent, ("gx", "gy"), split_axis=1, concat_axis=1, tiled=True)
    got = got.reshape(slices, grid_x, grid_y * rows, width)

    pitch = channels + 8
    return pl.pallas_call(
        functools.partial(
            back_kernel,
            grid_x=grid_x,
            rows_x=rows_x,
            channels=channels,
            pitch=pitch,
            per_device=per_device,
        ),
        grid=(slices,),
        in_specs=[
            pl.BlockSpec((1, grid_x, grid_y * rows, width), lambda t: (t, 0, 0, 0)),
            pl.BlockSpec(ymat.shape, lambda t: (0, 0)),
            pl.BlockSpec(xmat.shape, lambda t: (0, 0)),
        ],
        out_specs=pl.BlockSpec(
            (1, channels, per_device, extent, 2 * extent), lambda t: (t, 0, 0, 0, 0)
        ),
        out_shape=jax.ShapeDtypeStruct(
            (slices, channels, per_device, extent, 2 * extent), jnp.float32
        ),
        scratch_shapes=[
            pltpu.VMEM((ymat.shape[1] // LANES, grid_x, rows_x * pitch, LANES), jnp.float32)
        ],
        name="back",
    )(got, ymat, xmat)


def solution(mesh):
    return jax.shard_map(
        body,
        mesh=mesh,
        in_specs=(P("ta", None, None, None, None, None, "gx", "gy"), P()),
        out_specs=P("ta", None, ("gx", "gy"), None, None),
        check_vma=False,
    )
```

```python
import functools
import math

import jax
import jax.numpy as jnp
import numpy as np
from jax import lax
from jax.experimental import pallas as pl
from jax.experimental.pallas import tpu as pltpu
from jax.sharding import PartitionSpec as P

LANES = 128
SPINS = 4
PAIRS = SPINS * SPINS
SLOTS = PAIRS * PAIRS


def dft_tables(length):
    index = np.arange(length)
    angles = (index[:, None] * index[None, :] % length) * (2.0 * math.pi / length)
    norm = 1.0 / math.sqrt(length)
    return np.cos(angles) * norm, np.sin(angles) * norm


def z_matrix(length, lane_rows, per_device):
    cosine, sine = dft_tables(length)
    mix = np.array([[cosine, sine], [-sine, cosine]])
    eye = np.eye(lane_rows)
    full = np.einsum("oizk,yv->koyivz", mix, eye)
    return full.reshape(length * 2 * lane_rows, 2 * lane_rows * length)


def y_matrix(length, grid_y, steps, lane_rows, per_device):
    cosine, sine = dft_tables(length)
    cosine = cosine.reshape(grid_y, steps, lane_rows, length)
    sine = sine.reshape(grid_y, steps, lane_rows, length)
    real = np.stack([cosine, sine])
    imag = np.stack([-sine, cosine])
    plain = np.stack([real, imag])
    turned = np.stack([imag, -real])
    both = np.stack([plain, turned])
    full = np.einsum("aoigjvk,pq->gjpivaqok", both, np.eye(per_device))
    rows = grid_y * steps * per_device * 2 * lane_rows
    return full.reshape(rows, 2 * per_device * 2 * length)


def density_weights(table):
    count = table.shape[0]
    slot = lax.broadcasted_iota(jnp.int32, (count, SLOTS), 1)
    first, step = slot >> 4, slot & 15
    is_real = (step < 8) | ((step == 8) & (first < 8))
    second = (first + jnp.where(step > 8, step - 8, step)) & 15
    s1, s2, s3, s4 = first >> 2, first & 3, second >> 2, second & 3

    def pick(spin, base):
        value = jnp.broadcast_to(table[:, base : base + 1], (count, SLOTS))
        for q in range(1, SPINS):
            other = jnp.broadcast_to(table[:, base + q : base + q + 1], (count, SLOTS))
            value = jnp.where(spin == q, other, value)
        return value

    def weight(a1, a2, b1, b2):
        hit = (a1 == pick(b1, 0)) & (b2 == pick(a2, 0))
        code = (pick(b1, SPINS) + pick(a2, SPINS)) & 3
        real = jnp.where(code == 0, 1.0, 0.0) - jnp.where(code == 2, 1.0, 0.0)
        imag = jnp.where(code == 1, 1.0, 0.0) - jnp.where(code == 3, 1.0, 0.0)
        return jnp.where(hit, real, 0.0), jnp.where(hit, imag, 0.0)

    here_r, here_i = weight(s1, s2, s3, s4)
    swap_r, swap_i = weight(s3, s4, s1, s2)
    single = step == 0
    real = jnp.where(single, here_r, jnp.where(is_real, here_r + swap_r, swap_i - here_i))
    imag = jnp.where(single, here_i, jnp.where(is_real, here_i + swap_i, here_r - swap_r))
    return jnp.concatenate([real, imag], axis=0)


def front_kernel(prop, table, zmat, out, weights, turned, gram, *, tiles, colors, rows_x, owners):
    @pl.when((pl.program_id(0) == 0) & (pl.program_id(1) == 0))
    def _():
        weights[...] = density_weights(jnp.transpose(table[...])).astype(jnp.bfloat16)

    channels = weights.shape[0] // 2
    spread = colors * colors

    def narrow(part, s1, s2, color):
        c1, c2 = divmod(color, colors)
        wide = prop[0, part, s1, c1, s2, c2, :, :].astype(jnp.float32)
        halves = [wide[:, k * LANES : (k + 1) * LANES] for k in range(tiles)]
        return jnp.concatenate(halves, axis=0).astype(jnp.bfloat16)

    for pair in range(PAIRS):
        for color in range(spread):
            turned[pair, color] = -narrow(0, *divmod(pair, SPINS), color)

    def row(a, carry):
        def load(part, pair):
            s1, s2 = pair >> 2, pair & 3
            return [narrow(part, s1, s2, color).astype(jnp.float32) for color in range(spread)]

        def total(left, right):
            acc = left[0] * right[0]
            for x, y in zip(left[1:], right[1:]):
                acc = acc + x * y
            return acc

        def put(d, value):
            start = (a * PAIRS + d) * (rows_x + 1)
            for tile in range(tiles):
                gram[tile, pl.ds(start, rows_x), :] = value[tile * rows_x : (tile + 1) * rows_x]

        ar, ai = load(0, a), load(1, a)
        an = [turned[a, color].astype(jnp.float32) for color in range(spread)]
        put(0, total(ar + ai, ar + ai))
        for d in range(1, PAIRS // 2 + 1):
            b = (a + d) & (PAIRS - 1)
            br, bi = load(0, b), load(1, b)
            real, imag = total(ar + ai, br + bi), total(ai + an, br + bi)
            if d < PAIRS // 2:
                put(d, real)
                put(d + PAIRS // 2, imag)
            else:
                put(d, jnp.where(a < PAIRS // 2, real, imag))
        return carry

    lax.fori_loop(0, PAIRS, row, 0, unroll=2)

    pieces = []
    for tile in range(tiles):
        for x in range(rows_x):
            products = gram[tile, pl.ds(x, SLOTS, stride=rows_x + 1), :].astype(jnp.bfloat16)
            dens = jnp.dot(weights[...], products, preferred_element_type=jnp.float32)
            dens = dens.astype(jnp.bfloat16)
            pieces.append(jnp.concatenate([dens[:channels], dens[channels:]], axis=1))
    stacked = jnp.concatenate(pieces, axis=0)
    spread_z = lax.dot_general(
        zmat[...], stacked, (((1,), (1,)), ((), ())), preferred_element_type=jnp.float32
    )
    width = rows_x * channels
    rows = spread_z.shape[0] // owners
    spread_z = spread_z.reshape(owners, rows, tiles * width)
    out[0] = jnp.concatenate(
        [spread_z[:, :, k * width : (k + 1) * width] for k in range(tiles)], axis=1
    ).astype(jnp.bfloat16)


def back_kernel(data, ymat, xmat, out, lined, *, grid_x, rows_x, channels, pitch, per_device):
    cols = ymat.shape[1]
    blocks = cols // LANES
    for gx in range(grid_x):
        turned = lax.dot_general(
            data[0, gx], ymat[...], (((0,), (0,)), ((), ())), preferred_element_type=jnp.float32
        )
        for block in range(blocks):
            for x in range(rows_x):
                lined[block, gx, pl.ds(x * pitch, channels), :] = turned[
                    x * channels : (x + 1) * channels, block * LANES : (block + 1) * LANES
                ]
    for c in range(channels):
        sides = []
        for block in range(blocks):
            lines = [
                lined[block, gx, pl.ds(c, rows_x, stride=pitch), :] for gx in range(grid_x)
            ]
            sides.append(jnp.concatenate(lines, axis=0).astype(jnp.bfloat16))
        half = blocks // 2
        right = jnp.concatenate(
            [jnp.concatenate(sides[:half], axis=1), jnp.concatenate(sides[half:], axis=1)], axis=0
        )
        spectrum = jnp.dot(xmat[...], right, preferred_element_type=jnp.float32)
        width = cols // 2 // per_device
        for k in range(per_device):
            out[0, c, k] = spectrum[:, k * width : (k + 1) * width]


def body(propagator, gamma_table):
    slices, _, _, colors, _, _, rows_x, cols_yz = propagator.shape
    channels = gamma_table.shape[0]
    grid_x, grid_y = lax.axis_size("gx"), lax.axis_size("gy")
    owners = grid_x * grid_y
    extent = rows_x * grid_x
    per_device = extent // owners
    lane_rows = LANES // extent
    steps = cols_yz // LANES
    tiles = 2
    zmat = jnp.asarray(z_matrix(extent, lane_rows, per_device), jnp.bfloat16)
    ymat = jnp.asarray(y_matrix(extent, grid_y, steps, lane_rows, per_device), jnp.bfloat16)
    cosine, sine = dft_tables(extent)
    xmat = jnp.asarray(np.concatenate([cosine.T, sine.T], axis=1), jnp.bfloat16)

    width = rows_x * channels
    rows = steps * per_device * 2 * lane_rows
    step_rows = tiles * per_device * 2 * lane_rows
    sent = pl.pallas_call(
        functools.partial(
            front_kernel, tiles=tiles, colors=colors, rows_x=rows_x, owners=owners
        ),
        grid=(slices, steps // tiles),
        in_specs=[
            pl.BlockSpec(
                (1, 2, SPINS, colors, SPINS, colors, rows_x, tiles * LANES),
                lambda t, j: (t, 0, 0, 0, 0, 0, 0, j),
            ),
            pl.BlockSpec(gamma_table.shape[::-1], lambda t, j: (0, 0)),
            pl.BlockSpec(zmat.shape, lambda t, j: (0, 0)),
        ],
        out_specs=pl.BlockSpec((1, owners, step_rows, width), lambda t, j: (t, 0, j, 0)),
        out_shape=jax.ShapeDtypeStruct((slices, owners, rows, width), jnp.bfloat16),
        scratch_shapes=[
            pltpu.VMEM((2 * channels, SLOTS), jnp.bfloat16),
            pltpu.VMEM((PAIRS, colors * colors, tiles * rows_x, LANES), jnp.bfloat16),
            pltpu.VMEM((tiles, SLOTS * (rows_x + 1), LANES), jnp.float32),
        ],
        name="front",
    )(propagator, gamma_table.T, zmat)

    got = lax.all_to_all(sent, ("gx", "gy"), split_axis=1, concat_axis=1, tiled=True)
    got = got.reshape(slices, grid_x, grid_y * rows, width)

    pitch = channels + 8
    return pl.pallas_call(
        functools.partial(
            back_kernel,
            grid_x=grid_x,
            rows_x=rows_x,
            channels=channels,
            pitch=pitch,
            per_device=per_device,
        ),
        grid=(slices,),
        in_specs=[
            pl.BlockSpec((1, grid_x, grid_y * rows, width), lambda t: (t, 0, 0, 0)),
            pl.BlockSpec(ymat.shape, lambda t: (0, 0)),
            pl.BlockSpec(xmat.shape, lambda t: (0, 0)),
        ],
        out_specs=pl.BlockSpec(
            (1, channels, per_device, extent, 2 * extent), lambda t: (t, 0, 0, 0, 0)
        ),
        out_shape=jax.ShapeDtypeStruct(
            (slices, channels, per_device, extent, 2 * extent), jnp.float32
        ),
        scratch_shapes=[
            pltpu.VMEM((ymat.shape[1] // LANES, grid_x, rows_x * pitch, LANES), jnp.float32)
        ],
        name="back",
    )(got, ymat, xmat)


def solution(mesh):
    return jax.shard_map(
        body,
        mesh=mesh,
        in_specs=(P("ta", None, None, None, None, None, "gx", "gy"), P()),
        out_specs=P("ta", None, ("gx", "gy"), None, None),
        check_vma=False,
    )
```
